256 devices in a mesh: groups: 4 (over x, y), row: 64 (over z, core).
Axes of the slice: x: 2, y: 2, z: 32, core: 2. Of those that a mesh axis runs over, the one named last changes fastest.
The devices are a block of a 4x8x32 slice.
Arguments:
- factor_b: bfloat16 [64, 1048576], P(None, ('groups', 'row')), parts along dimension 1, may hold values from -12 to 12
- factor_c: bfloat16 [64, 1048576], P(None, ('groups', 'row')), parts along dimension 1, may hold values from -12 to 12
- sample_j: int32 [2097152], P(('groups', 'row')), parts along dimension 0, may hold values from 0 to 262143, as said below
- sample_k: int32 [64, 256, 128], P(None, ('groups', 'row')), parts along dimension 1, may hold values from 0 to 262143, as said below
- sample_weight: float32 [2097152], P(('groups', 'row')), parts along dimension 0, may hold values from 0.5 to 3.5
- block_values: bfloat16 [256, 64, 4, 4, 128], P(('groups', 'row')), parts along dimension 0, may hold values from -24 to 24
- block_sample: int32 [256, 64, 4, 4], P(('groups', 'row')), parts along dimension 0, may hold values from 0 to 8191
- block_count: int32 [256, 64, 4, 4], P(('groups', 'row')), parts along dimension 0, may hold values from 0 to 128, as said below
Outputs:
- factor_new: bfloat16 [64, 131072], P(None, ('groups', 'row')), parts along dimension 1
- scales: float32 [256], P('groups'), parts along dimension 0
The draws below stay inside these ranges and needn't reach their ends.
There are 4 independent parts, one for each index of `groups`. The reference program is written for one: setup_inputs(seed, part) draws one part's arguments, and reference() takes and returns one part's arrays. A program takes and returns all parts, laid end to end along the dimension named above; each array names one. Nothing has to cross between parts.
Inputs may be any that keep to these rules, and one draw needn't show every extreme that they name: sample_j[s] lies in rows s // 8192 * 4096 to s // 8192 * 4096 + 4095. sample_k[d, e, i] is the third-mode index of sample d * 8192 + e * 128 + i and lies in rows e * 4096 to e * 4096 + 4095. `block_count`: 0 marks an empty slot; slot [p, p, 0, 0] holds 128 for every p.
All inputs are finite; a program needn't handle non-finite values.
Results may differ from the reference program's by a relative error of at most 0.0051.
Values may be sent and summed in bfloat16 or wider, within the bound.
A program may use at most 64 MiB of HBM per device.

```python
import math
import jax
import jax.numpy as jnp
from jax import lax

R = 64
JD = 4096
KD = 4096
S_DEV = 8192
TD = 4
CT = 4
SPN = 128
S = 524288
J = 262144
K = 262144
I = 32768
N_ROW = 64


def factor_draw(key, total_rows):
    key_scale = jax.random.fold_in(key, 11)
    key_own = jax.random.fold_in(key, 12)
    key_spread = jax.random.fold_in(key, 14)
    column_scale = jnp.exp(jax.random.uniform(key_scale, (R, 1), minval=-math.log(1.5), maxval=math.log(1.5)))
    heavy_column = jax.random.randint(key_spread, (1, total_rows), 0, 128, dtype=jnp.int32) == 0
    spread_factor = jnp.where(heavy_column, 5.5, 0.8).astype(jnp.float32)
    own_part = jax.random.normal(key_own, (R, total_rows), dtype=jnp.float32)
    return (jnp.clip(own_part * spread_factor, -8.0, 8.0) * column_scale).astype(jnp.bfloat16)


def draw_factor_b(key, part):
    return factor_draw(jax.random.fold_in(key, 1), J)


def draw_factor_c(key, part):
    return factor_draw(jax.random.fold_in(key, 2), K)


def draw_sample_j(key, part):
    owner_block = jnp.arange(S, dtype=jnp.int32) // S_DEV
    offsets = jax.random.randint(jax.random.fold_in(key, 3), (S,), 0, JD, dtype=jnp.int32)
    return owner_block * JD + offsets


def draw_sample_k(key, part):
    holder = lax.broadcasted_iota(jnp.int32, (N_ROW, N_ROW, SPN), 1)
    offsets = jax.random.randint(jax.random.fold_in(key, 4), (N_ROW, N_ROW, SPN), 0, KD, dtype=jnp.int32)
    return holder * KD + offsets


def draw_sample_weight(key, part):
    device_pos = (jnp.arange(S, dtype=jnp.int32) // S_DEV).astype(jnp.float32)
    lift = jnp.sqrt(1.0 + 2.0 * device_pos / (N_ROW - 1))
    key_base = jax.random.fold_in(key, 5)
    base_weight = jnp.exp(jax.random.uniform(key_base, (S,), minval=-math.log(2.0), maxval=math.log(2.0)))
    return base_weight * lift


def draw_block_values(key, part):
    slot_shape = (N_ROW, N_ROW, TD, CT, 128)
    target = lax.broadcasted_iota(jnp.int32, slot_shape, 1).astype(jnp.float32)
    target_scale = 1.0 + 2.0 * target / (N_ROW - 1)
    key_noise = jax.random.fold_in(key, 6)
    noise_field = jax.random.normal(key_noise, slot_shape, dtype=jnp.float32)
    return (jnp.clip(noise_field, -8.0, 8.0) * target_scale).astype(jnp.bfloat16)


def draw_block_count(key, part):
    slot_shape = (N_ROW, N_ROW, TD, CT)
    source_ids = lax.broadcasted_iota(jnp.int32, slot_shape, 0)
    target_ids = lax.broadcasted_iota(jnp.int32, slot_shape, 1)
    tile_ids = lax.broadcasted_iota(jnp.int32, slot_shape, 2)
    slot_ids = lax.broadcasted_iota(jnp.int32, slot_shape, 3)
    fill_level = jax.random.randint(jax.random.fold_in(key, 7), (N_ROW,), 5, 9, dtype=jnp.int32)
    live_slot = jax.random.randint(jax.random.fold_in(key, 8), slot_shape, 0, 8, dtype=jnp.int32) < fill_level[None, :, None, None]
    most_live = 43 + 85 * source_ids // (N_ROW - 1)
    least_live = most_live // 2
    raw_count = jax.random.randint(jax.random.fold_in(key, 9), slot_shape, 0, 1 << 20, dtype=jnp.int32) % (most_live - least_live) + least_live + 1
    counted = jnp.where(live_slot, raw_count, jnp.zeros_like(raw_count))
    fixed_slot = (source_ids == target_ids) & (tile_ids == 0) & (slot_ids == 0)
    return jnp.where(fixed_slot, jnp.full_like(counted, 128), counted)


def place_ends(drawn, own_key, smallest, top_value):
    place = [jax.random.randint(jax.random.fold_in(own_key, axis), (), 0, length) for axis, length in enumerate(drawn.shape)]
    main_axis = drawn.shape.index(max(drawn.shape))
    beside = place[:main_axis] + [(place[main_axis] + 1) % drawn.shape[main_axis]] + place[main_axis + 1:]
    return drawn.at[tuple(place)].set(smallest).at[tuple(beside)].set(top_value)


def setup_inputs(seed: int = 0, part: int = 0) -> dict:
    key_list = jax.random.split(jax.random.key(seed), 9)
    own_keys = jax.random.split(jax.random.fold_in(key_list[8], part), 9)
    return {
        "factor_b": draw_factor_b(jax.random.fold_in(jax.random.fold_in(key_list[8], part), 71), part),
        "factor_c": draw_factor_c(jax.random.fold_in(jax.random.fold_in(key_list[8], part), 71), part),
        "sample_j": draw_sample_j(jax.random.fold_in(jax.random.fold_in(key_list[8], part), 71), part),
        "sample_k": draw_sample_k(jax.random.fold_in(jax.random.fold_in(key_list[8], part), 71), part),
        "sample_weight": draw_sample_weight(jax.random.fold_in(jax.random.fold_in(key_list[8], part), 71), part),
        "block_values": draw_block_values(jax.random.fold_in(jax.random.fold_in(key_list[8], part), 71), part),
        "block_sample": place_ends(jax.random.randint(own_keys[6], (N_ROW, N_ROW, TD, CT), 0, S_DEV), jax.random.fold_in(own_keys[6], 1), 0, S_DEV - 1).astype(jnp.int32),
        "block_count": draw_block_count(jax.random.fold_in(jax.random.fold_in(key_list[8], part), 71), part),
    }


def reference(factor_b, factor_c, sample_j, sample_k, sample_weight, block_values, block_sample, block_count):
    rank_width = factor_b.shape[0]
    b_columns = jnp.take(factor_b, sample_j, axis=1).astype(jnp.float32)
    c_columns = jnp.take(factor_c, sample_k.reshape(-1), axis=1).astype(jnp.float32)
    sketch = sample_weight[None, :] * b_columns * c_columns
    gram_matrix = jnp.dot(sketch, sketch.T, precision=lax.Precision.HIGHEST)
    live_total = jnp.sum(block_count.astype(jnp.float32))
    ridge = 0.05 * live_total / I
    system = gram_matrix / S + ridge * jnp.eye(rank_width, dtype=jnp.float32)
    lower_factor = jnp.linalg.cholesky(system)
    weighted = (sample_weight[None, :] * sketch).astype(jnp.bfloat16)
    positions = lax.broadcasted_iota(jnp.int32, block_values.shape, 4)
    masked = jnp.where(positions < block_count[..., None], block_values, jnp.zeros_like(block_values))
    owners = lax.broadcasted_iota(jnp.int32, block_sample.shape, 0) * S_DEV + block_sample
    picked = jnp.take(weighted, owners.reshape(-1).astype(jnp.int32), axis=1)
    picked = picked.reshape((rank_width,) + block_sample.shape)
    gathered = jnp.einsum('pqtcr,kpqtc->kqtr', masked.astype(jnp.float32), picked.astype(jnp.float32), precision=lax.Precision.HIGHEST).reshape(rank_width, -1)
    half_solved = lax.linalg.triangular_solve(lower_factor, gathered, left_side=True, lower=True)
    update = lax.linalg.triangular_solve(lower_factor, half_solved, left_side=True, lower=True, transpose_a=True)
    column_sums = lax.optimization_barrier(jnp.sum(update * update, axis=1))
    scales = jnp.sqrt(column_sums / I + 1e-06)
    return ((update / scales[:, None]).astype(jnp.bfloat16), scales)
```

```python
import functools

import jax
import jax.numpy as jnp
from jax import lax
from jax.experimental import pallas as pl
from jax.experimental.pallas import tpu as pltpu
from jax.sharding import PartitionSpec as P

MESH = pl.DeviceIdType.MESH
GROUPS_ROW = ("groups", "row")
HIGHEST = lax.Precision.HIGHEST
F32 = jnp.float32
BF16 = jnp.bfloat16


def partner(step, me, n, sign):
    chips = n // 2
    z, core = me // 2, me % 2
    rest = step - 2
    dist = jnp.where(step < 2, chips // 2, chips // 2 - 1 - rest // 4)
    way = jnp.where(step < 2, 1, 1 - 2 * ((rest // 2) % 2)) * sign
    other = jnp.where(step < 2, step, rest % 2)
    other = jnp.where(step == n - 2, 1 - core, other)
    return lax.rem(z + dist * way + chips, chips) * 2 + other


def send(src, dst, send_sem, recv_sem, peer):
    copy = pltpu.make_async_remote_copy(
        src_ref=src,
        dst_ref=dst,
        send_sem=send_sem,
        recv_sem=recv_sem,
        device_id={"row": peer},
        device_id_type=MESH,
    )
    copy.start()


def arrived(ref, send_sem, recv_sem, peer):
    pltpu.make_async_remote_copy(
        src_ref=ref, dst_ref=ref, send_sem=send_sem, recv_sem=recv_sem, device_id={"row": peer}, device_id_type=MESH
    ).wait_recv()


def sent(ref, send_sem, recv_sem, peer):
    pltpu.make_async_remote_copy(
        src_ref=ref, dst_ref=ref, send_sem=send_sem, recv_sem=recv_sem, device_id={"row": peer}, device_id_type=MESH
    ).wait_send()


def kernel(
    n,
    total_samples,
    total_rows,
    k_ref,
    j_ref,
    pick_ref,
    live_ref,
    b_ref,
    c_ref,
    w_ref,
    values_ref,
    out_ref,
    scales_ref,
    table_c,
    table_b,
    stage,
    c_out,
    c_in,
    wb,
    wp,
    wk,
    values_in,
    rows_out,
    rows_in,
    g_out,
    g_one,
    g_mid,
    g_two,
    g_sum,
    g_all,
    s_out,
    s_one,
    s_mid,
    s_two,
    c_send,
    c_recv,
    v_send,
    v_recv,
    r_send,
    r_recv,
    small_send,
    small_recv,
):
    me = lax.axis_index("row")
    rank = b_ref.shape[0]
    depth_c, depth_b = c_ref.shape[1], b_ref.shape[1]
    per = k_ref.shape[0] // n
    half = per // 2
    side = 8
    assert depth_c & (depth_c - 1) == 0 and depth_b & (depth_b - 1) == 0
    ring, seat = me // side, me % side
    lane = lax.broadcasted_iota(jnp.int32, (1, 128), 1)
    left = lane < rank

    barrier = pltpu.get_barrier_semaphore()

    def greet(i, _):
        pl.semaphore_signal(barrier, inc=1, device_id={"row": partner(i, me, n, 1)}, device_id_type=MESH)
        return 0

    lax.fori_loop(0, n - 1, greet, 0)

    def fill(table, ref):
        def chunk(i, _):
            at = pl.multiple_of(i * 128, 128)
            part = ref[:, pl.ds(at, 128)].astype(F32).T
            table[pl.ds(at, 128), :] = jnp.concatenate([part, part], axis=1)
            return 0

        lax.fori_loop(0, ref.shape[1] // 128, chunk, 0)

    def rows_of(table, index_ref, at, mask):
        for i in range(half):
            first = table[pl.ds(index_ref[at + i] & mask, 1), :]
            second = table[pl.ds(index_ref[at + half + i] & mask, 1), :]
            stage[i : i + 1, :] = jnp.where(left, first, second)
        return stage[...]

    fill(table_c, c_ref)

    def gather_c(i, _):
        peer = jnp.where(i == n - 1, me, partner(i, me, n, 1))
        c_out[peer] = rows_of(table_c, k_ref, peer * per, depth_c - 1).astype(BF16)
        return 0

    early = n // 2
    lax.fori_loop(0, early, gather_c, 0)

    pl.semaphore_wait(barrier, n - 1)

    def send_values(i, _):
        peer = partner(i, me, n, 1)
        send(values_ref.at[peer], values_in.at[me], v_send.at[peer], v_recv.at[me], peer)
        return 0

    lax.fori_loop(0, n - 1, send_values, 0)
    lax.fori_loop(early, n, gather_c, 0)

    def send_c(i, _):
        peer = partner(i, me, n, 1)
        send(c_out.at[peer], c_in.at[me], c_send.at[peer], c_recv.at[me], peer)
        return 0

    lax.fori_loop(0, n - 1, send_c, 0)
    values_in[me] = values_ref[me]

    fill(table_b, b_ref)

    def weigh(i, _):
        turned = w_ref[pl.ds(pl.multiple_of(i * 8, 8), 8), :].T
        for j in range(8):
            wp[i * 8 + j] = jnp.where(left, turned[:half, j : j + 1], turned[half:, j : j + 1])
        return 0

    lax.fori_loop(0, n // 8, weigh, 0)

    def gather_b(e, _):
        wb[e] = rows_of(table_b, j_ref, e * per, depth_b - 1) * wp[e]
        return 0

    lax.fori_loop(0, n, gather_b, 0)

    def use(e, c_rows, gram):
        sketch = wb[e] * c_rows.astype(F32)
        weighted = wp[e] * sketch
        turned = pltpu.roll(weighted, rank, 1)
        at = pl.multiple_of(e * per, 128)
        wk[pl.ds(at, half), :] = jnp.where(left, weighted, turned)
        wk[pl.ds(at + half, half), :] = jnp.where(left, turned, weighted)
        return gram + lax.dot_general(
            sketch, sketch, (((0,), (0,)), ((), ())), precision=HIGHEST, preferred_element_type=F32
        )

    gram = use(me, c_out[me], jnp.zeros((128, 128), F32))

    def take(i, gram):
        e = partner(i, me, n, -1)
        arrived(c_in.at[e], c_send.at[e], c_recv.at[e], e)
        return use(e, c_in[e], gram)

    gram = lax.fori_loop(0, n - 1, take, gram)

    eye = lax.broadcasted_iota(jnp.int32, (rank, 128), 0) == lax.broadcasted_iota(jnp.int32, (rank, 128), 1)
    square = gram[:rank, :rank] + gram[rank:, rank:]
    ridge = (0.05 / total_rows) * live_ref[0]
    system = square * (1.0 / total_samples) + jnp.where(eye[:, :rank], ridge, 0.0)
    packed = jnp.concatenate([system[: rank // 2], system[rank // 2 :]], axis=1)
    lines = packed.shape[0] // side
    for i in range(side):
        g_out[i] = packed[i * lines : (i + 1) * lines]
    g_one[seat] = g_out[seat]

    def spread(kind, src_of, dst, peer_of, own):
        for j in range(1, side):
            peer, index = peer_of(j)
            send(src_of(index), dst.at[own], small_send.at[kind, index], small_recv.at[kind, own], peer)

    def collect(kind, dst, peer_of):
        for j in range(1, side):
            peer, index = peer_of(j)
            arrived(dst.at[index], small_send.at[kind, index], small_recv.at[kind, index], peer)

    def in_ring(j):
        index = lax.rem(seat + j, side)
        return ring * side + index, index

    def across(j):
        index = lax.rem(ring + j, side)
        return index * side + seat, index

    spread(0, lambda i: g_out.at[i], g_one, in_ring, seat)

    def pick(q, _):
        at = q * 16
        for i in range(8):
            first = wk[pl.ds(pick_ref[at + i], 1), :]
            second = wk[pl.ds(pick_ref[at + 8 + i], 1), :]
            stage[i : i + 1, :] = jnp.where(left, first, second)
        rows_out[q] = stage[0:8, :].astype(BF16)
        return 0

    lax.fori_loop(0, n, pick, 0)

    collect(0, g_one, in_ring)
    total = g_one[0]
    for i in range(1, side):
        total = total + g_one[i]
    g_mid[...] = total
    g_two[ring] = total
    spread(1, lambda i: g_mid, g_two, across, ring)

    def send_rows(i, _):
        peer = partner(i, me, n, 1)
        send(rows_out.at[peer], rows_in.at[me], r_send.at[peer], r_recv.at[me], peer)
        return 0

    lax.fori_loop(0, n - 1, send_rows, 0)
    rows_in[me] = rows_out[me]

    collect(1, g_two, across)
    total = g_two[0]
    for i in range(1, side):
        total = total + g_two[i]
    g_sum[...] = total
    g_all[seat] = total
    spread(2, lambda i: g_sum, g_all, in_ring, seat)
    collect(2, g_all, in_ring)
    packed = jnp.concatenate([g_all[i] for i in range(side)], axis=0)
    matrix = jnp.concatenate([packed, pltpu.roll(packed, rank, 1)], axis=0)
    matrix = jnp.where(left, matrix, pltpu.roll(matrix, rank, 1))

    row_at = lax.broadcasted_iota(jnp.int32, (rank, 1), 0)
    lane_at = lax.rem(lane, rank)

    def eliminate(_, m):
        for i in range(8):
            column = m[:, i : i + 1]
            inverse = 1.0 / m[i : i + 1, i : i + 1]
            line = jnp.where(lane_at == i, 1.0, m[i : i + 1, :]) * inverse
            rest = jnp.where(lane_at == i, 0.0, m) - column * line
            m = jnp.where(row_at == i, line, rest)
        m = pltpu.roll(m, 120, 1)
        return jnp.concatenate([m[8:], m[:8]], axis=0)

    inverse = lax.fori_loop(0, rank // 8, eliminate, matrix)[:, :rank]

    def wait_blocks(i, _):
        e = partner(i, me, n, -1)
        arrived(values_in.at[e], v_send.at[e], v_recv.at[e], e)
        arrived(rows_in.at[e], r_send.at[e], r_recv.at[e], e)
        return 0

    lax.fori_loop(0, n - 1, wait_blocks, 0)

    rows = rows_in[...].astype(F32).reshape(n * 8, 128)
    low = values_in[:, 0].astype(F32).reshape(n * 8, 128).astype(BF16)
    high = values_in[:, 1].astype(F32).reshape(n * 8, 128).astype(BF16)
    slot = lax.rem(lax.broadcasted_iota(jnp.int32, (n * 8, 1), 0), 8)

    def mixed(mask, values):
        return lax.dot_general(
            jnp.where(mask, rows, 0.0).astype(BF16), values, (((0,), (0,)), ((), ())), preferred_element_type=F32
        )

    gathered = [
        mixed(slot < 4, low)[:rank],
        mixed(slot >= 4, low)[:rank],
        mixed(slot < 4, high)[rank:],
        mixed(slot >= 4, high)[rank:],
    ]
    update = [
        lax.dot_general(inverse, g, (((1,), (0,)), ((), ())), precision=HIGHEST, preferred_element_type=F32)
        for g in gathered
    ]
    squares = update[0] * update[0]
    for u in update[1:]:
        squares = squares + u * u
    own = jnp.sum(squares, axis=1, keepdims=True)
    own = jnp.sum(jnp.where(eye, own, 0.0), axis=0, keepdims=True)
    s_out[...] = own
    s_one[seat] = own
    spread(3, lambda i: s_out, s_one, in_ring, seat)
    collect(3, s_one, in_ring)
    total = s_one[0]
    for i in range(1, side):
        total = total + s_one[i]
    s_mid[...] = total
    s_two[ring] = total
    spread(4, lambda i: s_mid, s_two, across, ring)
    collect(4, s_two, across)
    total = s_two[0]
    for i in range(1, side):
        total = total + s_two[i]
    scales = jnp.sqrt(total / total_rows + 1e-06)
    scales_ref[...] = scales
    column = jnp.sum(jnp.where(eye, scales, 0.0), axis=1, keepdims=True)
    for t, u in enumerate(update):
        out_ref[:, t * 128 : (t + 1) * 128] = (u / column).astype(BF16)

    def drain(i, _):
        peer = partner(i, me, n, 1)
        sent(values_ref.at[peer], v_send.at[peer], v_recv.at[peer], peer)
        sent(c_out.at[peer], c_send.at[peer], c_recv.at[peer], peer)
        sent(rows_out.at[peer], r_send.at[peer], r_recv.at[peer], peer)
        return 0

    lax.fori_loop(0, n - 1, drain, 0)
    for kind, ref, peer_of in (
        (0, g_out.at[0], in_ring),
        (1, g_mid, across),
        (2, g_sum, in_ring),
        (3, s_out, in_ring),
        (4, s_mid, across),
    ):
        for j in range(1, side):
            peer, index = peer_of(j)
            sent(ref, small_send.at[kind, index], small_recv.at[kind, index], peer)


def solution(mesh):
    n = mesh.shape["row"]

    def shards(
        factor_b, factor_c, sample_j, sample_k, sample_weight, block_values, block_sample, block_count
    ):
        rank = factor_b.shape[0]
        samples = sample_j.shape[0]
        _, _, tiles, slots, width = block_values.shape
        positions = lax.broadcasted_iota(jnp.int32, block_values.shape, 4)
        masked = jnp.where(positions < block_count[..., None], block_values, jnp.zeros_like(block_values))
        masked = masked.reshape(n, 2, tiles * slots // 2, width)
        live = jnp.sum(block_count.astype(F32)).reshape(1)
        vmem = pl.BlockSpec(memory_space=pltpu.VMEM)
        smem = pl.BlockSpec(memory_space=pltpu.SMEM)
        half = samples // n // 2
        out, scales = pl.pallas_call(
            functools.partial(kernel, n, samples * n, tiles * width * n),
            out_shape=(
                jax.ShapeDtypeStruct((rank, tiles * width), BF16),
                jax.ShapeDtypeStruct((1, 128), F32),
            ),
            in_specs=[smem] * 4 + [vmem] * 4,
            out_specs=(vmem, vmem),
            scratch_shapes=[
                pltpu.VMEM((factor_c.shape[1], 128), F32),
                pltpu.VMEM((factor_b.shape[1], 128), F32),
                pltpu.VMEM((half, 128), F32),
                pltpu.VMEM((n, half, 128), BF16),
                pltpu.VMEM((n, half, 128), BF16),
                pltpu.VMEM((n, half, 128), F32),
                pltpu.VMEM((n, half, 128), F32),
                pltpu.VMEM((samples, 128), F32),
                pltpu.VMEM(masked.shape, BF16),
                pltpu.VMEM((n, 8, 128), BF16),
                pltpu.VMEM((n, 8, 128), BF16),
                pltpu.VMEM((8, 4, 128), F32),
                pltpu.VMEM((8, 4, 128), F32),
                pltpu.VMEM((4, 128), F32),
                pltpu.VMEM((8, 4, 128), F32),
                pltpu.VMEM((4, 128), F32),
                pltpu.VMEM((8, 4, 128), F32),
                pltpu.VMEM((1, 128), F32),
                pltpu.VMEM((8, 1, 128), F32),
                pltpu.VMEM((1, 128), F32),
                pltpu.VMEM((8, 1, 128), F32),
            ]
            + [pltpu.SemaphoreType.DMA((n,))] * 6
            + [pltpu.SemaphoreType.DMA((5, 8))] * 2,
            compiler_params=pltpu.CompilerParams(collective_id=0, has_side_effects=True),
            name="step",
        )(
            sample_k.reshape(-1),
            sample_j,
            block_sample.reshape(-1),
            live,
            factor_b,
            factor_c,
            sample_weight.reshape(n, -1),
            masked,
        )
        return out, scales[0, :rank]

    return jax.shard_map(
        shards,
        mesh=mesh,
        in_specs=(
            P(None, GROUPS_ROW),
            P(None, GROUPS_ROW),
            P(GROUPS_ROW),
            P(None, GROUPS_ROW, None),
            P(GROUPS_ROW),
            P(GROUPS_ROW, None, None, None, None),
            P(GROUPS_ROW, None, None, None),
            P(GROUPS_ROW, None, None, None),
        ),
        out_specs=(P(None, GROUPS_ROW), P("groups")),
        check_vma=False,
    )
```

```python
import functools

import jax
import jax.numpy as jnp
from jax import lax
from jax.experimental import pallas as pl
from jax.experimental.pallas import tpu as pltpu
from jax.sharding import PartitionSpec as P

MESH = pl.DeviceIdType.MESH
GROUPS_ROW = ("groups", "row")
HIGHEST = lax.Precision.HIGHEST
F32 = jnp.float32
BF16 = jnp.bfloat16


def partner(step, me, n, sign):
    chips = n // 2
    z, core = me // 2, me % 2
    rest = step - 2
    dist = jnp.where(step < 2, chips // 2, chips // 2 - 1 - rest // 4)
    way = jnp.where(step < 2, 1, 1 - 2 * ((rest // 2) % 2)) * sign
    other = jnp.where(step < 2, step, rest % 2)
    other = jnp.where(step == n - 2, 1 - core, other)
    return lax.rem(z + dist * way + chips, chips) * 2 + other


def send(src, dst, send_sem, recv_sem, peer):
    copy = pltpu.make_async_remote_copy(
        src_ref=src,
        dst_ref=dst,
        send_sem=send_sem,
        recv_sem=recv_sem,
        device_id={"row": peer},
        device_id_type=MESH,
    )
    copy.start()


def wait_blocks(ref, send_sem, recv_sem, peer, incoming):
    copy = pltpu.make_async_remote_copy(
        src_ref=ref, dst_ref=ref, send_sem=send_sem, recv_sem=recv_sem, device_id={"row": peer}, device_id_type=MESH
    )
    if incoming:
        copy.wait_recv()
    else:
        copy.wait_send()


def kernel(
    n,
    total_samples,
    total_rows,
    k_hbm,
    j_hbm,
    pick_hbm,
    count_hbm,
    b_hbm,
    c_hbm,
    w_hbm,
    values_hbm,
    update_hbm,
    scales_ref,
    k_ref,
    j_ref,
    pick_ref,
    count_ref,
    b_ref,
    c_ref,
    w_ref,
    values_ref,
    table_c,
    table_b,
    stage,
    c_out,
    c_in,
    wb,
    wp,
    wk,
    values_out,
    values_in,
    rows_out,
    rows_in,
    g_out,
    g_one,
    g_mid,
    g_two,
    g_sum,
    g_all,
    s_out,
    s_in,
    update_ref,
    local,
    c_recv,
    c_send,
    v_send,
    v_recv,
    r_send,
    r_recv,
    s_send,
    s_recv,
    small_send,
    small_recv,
):
    me = lax.axis_index("row")
    rank = b_ref.shape[0]
    depth_c, depth_b = c_ref.shape[1], b_ref.shape[1]
    per = k_ref.shape[0] // n
    half = per // 2
    side = 8
    assert depth_c & (depth_c - 1) == 0 and depth_b & (depth_b - 1) == 0
    ring, seat = me // side, me % side
    lane = lax.broadcasted_iota(jnp.int32, (1, 128), 1)
    left = lane < rank

    barrier = pltpu.get_barrier_semaphore()
    home = (me // 2) * 2

    def greet_chip(offset):
        chip = lax.rem(home + offset, n)
        for core in range(2):
            pl.semaphore_signal(barrier, inc=1, device_id={"row": chip + core}, device_id_type=MESH)

    def greet(i, _):
        greet_chip(n // 2 - 2 * i)
        greet_chip(n // 2 + 2 * i)
        return 0

    loads = [
        pltpu.make_async_copy(src, dst, local.at[i])
        for i, (src, dst) in enumerate(
            (
                (count_hbm, count_ref),
                (values_hbm, values_ref),
                (c_hbm, c_ref),
                (k_hbm, k_ref),
                (b_hbm, b_ref),
                (j_hbm, j_ref),
                (w_hbm, w_ref),
                (pick_hbm, pick_ref),
            )
        )
    ]
    for copy in loads:
        copy.start()
    pl.semaphore_signal(barrier, inc=1, device_id={"row": home + 1 - me % 2}, device_id_type=MESH)
    greet_chip(n // 2)
    lax.fori_loop(1, n // 4, greet, 0)

    loads[0].wait()
    loads[1].wait()
    counts = count_ref[...]
    live = jnp.sum(jnp.sum(counts.astype(F32), axis=1, keepdims=True), axis=0, keepdims=True)
    counts = jnp.concatenate([counts, counts], axis=1)

    def mask_values(peer):
        turned = pltpu.roll(counts, 128 - peer, 1)
        for part in range(2):
            kept = lane < turned[part * 8 : part * 8 + 8, 0:1]
            values_out[peer, part] = jnp.where(kept, values_ref[peer, part].astype(F32), 0.0).astype(BF16)

    def send_value(i):
        peer = partner(i, me, n, 1)
        send(values_out.at[peer], values_in.at[me], v_send, v_recv, peer)

    def both(i, _):
        mask_values(partner(i, me, n, 1))
        send_value(i - 1)
        return 0

    mask_values(me)
    values_in[me] = values_out[me]
    mask_values(partner(0, me, n, 1))
    pl.semaphore_wait(barrier, n - 1)
    lax.fori_loop(1, n - 1, both, 0)
    send_value(n - 2)

    def fill(table, ref):
        def chunk(i, _):
            at = pl.multiple_of(i * 128, 128)
            part = ref[:, pl.ds(at, 128)].astype(F32).T
            table[pl.ds(at, 128), :] = jnp.concatenate([part, part], axis=1)
            return 0

        lax.fori_loop(0, ref.shape[1] // 128, chunk, 0)

    def rows_of(table, index_ref, at, mask):
        for i in range(half):
            first = table[pl.ds(index_ref[at + i] & mask, 1), :]
            second = table[pl.ds(index_ref[at + half + i] & mask, 1), :]
            stage[i : i + 1, :] = jnp.where(left, first, second)
        return stage[...]

    loads[2].wait()
    fill(table_c, c_ref)
    loads[3].wait()

    def gather_c(i, _):
        peer = jnp.where(i == n - 1, me, partner(i, me, n, 1))
        c_out[peer] = rows_of(table_c, k_ref, peer * per, depth_c - 1).astype(BF16)
        return 0

    lax.fori_loop(0, n, gather_c, 0)

    def send_c(i, _):
        peer = partner(i, me, n, 1)
        send(c_out.at[peer], c_in.at[me], c_send, c_recv.at[me], peer)
        return 0

    lax.fori_loop(0, n - 1, send_c, 0)

    for copy in loads[4:]:
        copy.wait()
    fill(table_b, b_ref)

    def weigh(i, _):
        turned = w_ref[pl.ds(pl.multiple_of(i * 8, 8), 8), :].T
        for j in range(8):
            wp[i * 8 + j] = jnp.where(left, turned[:half, j : j + 1], turned[half:, j : j + 1])
        return 0

    lax.fori_loop(0, n // 8, weigh, 0)

    def gather_b(e, _):
        wb[e] = rows_of(table_b, j_ref, e * per, depth_b - 1) * wp[e]
        return 0

    lax.fori_loop(0, n, gather_b, 0)

    def use(e, c_rows, gram):
        sketch = wb[e] * c_rows.astype(F32)
        weighted = wp[e] * sketch
        turned = pltpu.roll(weighted, rank, 1)
        at = pl.multiple_of(e * per, 128)
        wk[pl.ds(at, half), :] = jnp.where(left, weighted, turned)
        wk[pl.ds(at + half, half), :] = jnp.where(left, turned, weighted)
        return gram + lax.dot_general(
            sketch, sketch, (((0,), (0,)), ((), ())), precision=HIGHEST, preferred_element_type=F32
        )

    gram = use(me, c_out[me], jnp.zeros((128, 128), F32))

    def take(i, gram):
        e = partner(i, me, n, -1)
        wait_blocks(c_in.at[e], c_send, c_recv.at[e], e, True)
        return use(e, c_in[e], gram)

    gram = lax.fori_loop(0, n - 1, take, gram)

    eye = lax.broadcasted_iota(jnp.int32, (rank, 128), 0) == lax.broadcasted_iota(jnp.int32, (rank, 128), 1)
    square = gram[:rank, :rank] + gram[rank:, rank:]
    system = square * (1.0 / total_samples) + jnp.where(eye[:, :rank], live * (0.05 / total_rows), 0.0)
    packed = jnp.concatenate([system[: rank // 2], system[rank // 2 :]], axis=1)
    lines = packed.shape[0] // side
    for i in range(side):
        g_out[i] = packed[i * lines : (i + 1) * lines]
    g_one[seat] = g_out[seat]

    def spread(kind, src_of, dst, peer_of, own):
        for j in range(1, side):
            peer, index = peer_of(j)
            send(src_of(index), dst.at[own], small_send.at[kind, index], small_recv.at[kind, own], peer)

    def collect(kind, dst, peer_of):
        for j in range(1, side):
            peer, index = peer_of(j)
            wait_blocks(dst.at[index], small_send.at[kind, index], small_recv.at[kind, index], peer, True)

    def in_ring(j):
        index = lax.rem(seat + j, side)
        return ring * side + index, index

    def across(j):
        index = lax.rem(ring + j, side)
        return index * side + seat, index

    def total_of(ref):
        total = ref[0]
        for i in range(1, side):
            total = total + ref[i]
        return total

    spread(0, lambda i: g_out.at[i], g_one, in_ring, seat)

    def pick(q, _):
        for i in range(8):
            first = wk[pl.ds(pick_ref[i, q], 1), :]
            second = wk[pl.ds(pick_ref[8 + i, q], 1), :]
            stage[i : i + 1, :] = jnp.where(left, first, second)
        rows_out[q] = stage[0:8, :].astype(BF16)
        return 0

    lax.fori_loop(0, n, pick, 0)

    collect(0, g_one, in_ring)
    total = total_of(g_one)
    g_mid[...] = total
    g_two[ring] = total
    spread(1, lambda i: g_mid, g_two, across, ring)

    def send_rows(i, _):
        peer = partner(i, me, n, 1)
        send(rows_out.at[peer], rows_in.at[me], r_send, r_recv, peer)
        return 0

    first_part = n * 5 // 8
    lax.fori_loop(0, first_part, send_rows, 0)
    rows_in[me] = rows_out[me]

    collect(1, g_two, across)
    total = total_of(g_two)
    g_sum[...] = total
    g_all[seat] = total
    spread(2, lambda i: g_sum, g_all, in_ring, seat)
    lax.fori_loop(first_part, n - 1, send_rows, 0)
    collect(2, g_all, in_ring)
    packed = jnp.concatenate([g_all[i] for i in range(side)], axis=0)
    matrix = jnp.concatenate([packed, pltpu.roll(packed, rank, 1)], axis=0)
    matrix = jnp.where(left, matrix, pltpu.roll(matrix, rank, 1))

    row_at = lax.broadcasted_iota(jnp.int32, (rank, 1), 0)
    lane_at = lax.rem(lane, rank)

    def eliminate(_, m):
        for i in range(8):
            column = jnp.broadcast_to(m[:, i : i + 1], m.shape)
            line = jnp.where(lane_at == i, 1.0, m[i : i + 1, :]) * (1.0 / column[i : i + 1, :])
            rest = jnp.where(lane_at == i, 0.0, m) - column * line
            m = jnp.where(row_at == i, line, rest)
        m = pltpu.roll(m, 120, 1)
        return jnp.concatenate([m[8:], m[:8]], axis=0)

    inverse = lax.fori_loop(0, rank // 8, eliminate, matrix)[:, :rank]

    far = lax.rem(me + n // 2, n)
    rest = pl.ds(0, n - 1)
    wait_blocks(values_in.at[rest], v_send, v_recv, far, True)
    wait_blocks(rows_in.at[rest], r_send, r_recv, far, True)

    rows = rows_in[...].astype(F32).reshape(n * 8, 128)
    low = values_in[:, 0].astype(F32).reshape(n * 8, 128).astype(BF16)
    high = values_in[:, 1].astype(F32).reshape(n * 8, 128).astype(BF16)
    slot = lax.rem(lax.broadcasted_iota(jnp.int32, (n * 8, 1), 0), 8)

    def mixed(mask, values):
        return lax.dot_general(
            jnp.where(mask, rows, 0.0).astype(BF16), values, (((0,), (0,)), ((), ())), preferred_element_type=F32
        )

    gathered = [
        mixed(slot < 4, low)[:rank],
        mixed(slot >= 4, low)[:rank],
        mixed(slot < 4, high)[rank:],
        mixed(slot >= 4, high)[rank:],
    ]
    squares = jnp.zeros((rank, 128), F32)
    for t, g in enumerate(gathered):
        u = lax.dot_general(inverse, g, (((1,), (0,)), ((), ())), precision=HIGHEST, preferred_element_type=F32)
        update_ref[:, t * 128 : (t + 1) * 128] = u
        squares = squares + u * u
    own = jnp.sum(squares, axis=1, keepdims=True)
    own = jnp.sum(jnp.where(eye, own, 0.0), axis=0, keepdims=True)
    s_out[...] = own
    s_in[me] = own

    def send_sums(i, _):
        peer = partner(i, me, n, 1)
        send(s_out, s_in.at[me], s_send, s_recv, peer)
        return 0

    lax.fori_loop(0, n - 1, send_sums, 0)
    leave = pltpu.make_async_copy(update_ref, update_hbm, local.at[len(loads)])
    leave.start()
    wait_blocks(values_out.at[rest], v_send, v_recv, far, False)
    wait_blocks(c_out.at[rest], c_send, c_recv.at[me], far, False)
    wait_blocks(rows_out.at[rest], r_send, r_recv, far, False)
    for kind, ref, peer_of in ((0, g_out.at[0], in_ring), (1, g_mid, across), (2, g_sum, in_ring)):
        for j in range(1, side):
            peer, index = peer_of(j)
            wait_blocks(ref, small_send.at[kind, index], small_recv.at[kind, index], peer, False)
    leave.wait()
    wait_blocks(s_in.at[rest], s_send, s_recv, far, False)
    wait_blocks(s_in.at[rest], s_send, s_recv, far, True)
    total = jnp.sum(s_in[...], axis=0)
    scales_ref[...] = jnp.sqrt(total / total_rows + 1e-06)


def solution(mesh):
    n = mesh.shape["row"]

    def shards(
        factor_b, factor_c, sample_j, sample_k, sample_weight, block_values, block_sample, block_count
    ):
        rank = factor_b.shape[0]
        samples = sample_j.shape[0]
        _, _, tiles, slots, width = block_values.shape
        values = block_values.reshape(n, 2, tiles * slots // 2, width)
        counts = block_count[0].transpose(1, 2, 0).reshape(tiles * slots, n)
        picks = block_sample[0].transpose(1, 2, 0).reshape(tiles * slots, n)
        weights = sample_weight.reshape(n, -1)
        vmem = pl.BlockSpec(memory_space=pltpu.VMEM)
        anywhere = pl.BlockSpec(memory_space=pl.ANY)
        half = samples // n // 2
        update, scales = pl.pallas_call(
            functools.partial(kernel, n, samples * n, tiles * width * n),
            out_shape=(
                jax.ShapeDtypeStruct((rank, tiles * width), F32),
                jax.ShapeDtypeStruct((1, 128), F32),
            ),
            in_specs=[anywhere] * 8,
            out_specs=(anywhere, vmem),
            scratch_shapes=[
                pltpu.SMEM((samples,), jnp.int32),
                pltpu.SMEM((samples,), jnp.int32),
                pltpu.SMEM(picks.shape, jnp.int32),
                pltpu.VMEM(counts.shape, jnp.int32),
                pltpu.VMEM(factor_b.shape, BF16),
                pltpu.VMEM(factor_c.shape, BF16),
                pltpu.VMEM(weights.shape, F32),
                pltpu.VMEM(values.shape, BF16),
                pltpu.VMEM((factor_c.shape[1], 128), F32),
                pltpu.VMEM((factor_b.shape[1], 128), F32),
                pltpu.VMEM((half, 128), F32),
                pltpu.VMEM((n, half, 128), BF16),
                pltpu.VMEM((n, half, 128), BF16),
                pltpu.VMEM((n, half, 128), F32),
                pltpu.VMEM((n, half, 128), F32),
                pltpu.VMEM((samples, 128), F32),
                pltpu.VMEM(values.shape, BF16),
                pltpu.VMEM(values.shape, BF16),
                pltpu.VMEM((n, 8, 128), BF16),
                pltpu.VMEM((n, 8, 128), BF16),
                pltpu.VMEM((8, 4, 128), F32),
                pltpu.VMEM((8, 4, 128), F32),
                pltpu.VMEM((4, 128), F32),
                pltpu.VMEM((8, 4, 128), F32),
                pltpu.VMEM((4, 128), F32),
                pltpu.VMEM((8, 4, 128), F32),
                pltpu.VMEM((1, 128), F32),
                pltpu.VMEM((n, 1, 128), F32),
                pltpu.VMEM((rank, tiles * width), F32),
                pltpu.SemaphoreType.DMA((9,)),
                pltpu.SemaphoreType.DMA((n,)),
            ]
            + [pltpu.SemaphoreType.DMA(())] * 7
            + [pltpu.SemaphoreType.DMA((3, 8))] * 2,
            compiler_params=pltpu.CompilerParams(collective_id=0, has_side_effects=True),
            name="step",
        )(
            sample_k.reshape(-1),
            sample_j,
            picks,
            counts,
            factor_b,
            factor_c,
            weights,
            values,
        )
        scales = scales[0, :rank]
        return (update / scales[:, None]).astype(BF16), scales

    return jax.shard_map(
        shards,
        mesh=mesh,
        in_specs=(
            P(None, GROUPS_ROW),
            P(None, GROUPS_ROW),
            P(GROUPS_ROW),
            P(None, GROUPS_ROW, None),
            P(GROUPS_ROW),
            P(GROUPS_ROW, None, None, None, None),
            P(GROUPS_ROW, None, None, None),
            P(GROUPS_ROW, None, None, None),
        ),
        out_specs=(P(None, GROUPS_ROW), P("groups")),
        check_vma=False,
    )
```

```python
import functools

import jax
import jax.numpy as jnp
from jax import lax
from jax.experimental import pallas as pl
from jax.experimental.pallas import tpu as pltpu
from jax.sharding import PartitionSpec as P

MESH = pl.DeviceIdType.MESH
GROUPS_ROW = ("groups", "row")
HIGHEST = lax.Precision.HIGHEST
F32 = jnp.float32
BF16 = jnp.bfloat16


def partner(step, me, n, sign):
    chips = n // 2
    z, core = me // 2, me % 2
    rest = step - 2
    dist = jnp.where(step < 2, chips // 2, chips // 2 - 1 - rest // 4)
    way = jnp.where(step < 2, 1, 1 - 2 * ((rest // 2) % 2)) * sign
    other = jnp.where(step < 2, step, rest % 2)
    other = jnp.where(step == n - 2, 1 - core, other)
    return lax.rem(z + dist * way + chips, chips) * 2 + other


def send(src, dst, send_sem, recv_sem, peer):
    copy = pltpu.make_async_remote_copy(
        src_ref=src,
        dst_ref=dst,
        send_sem=send_sem,
        recv_sem=recv_sem,
        device_id={"row": peer},
        device_id_type=MESH,
    )
    copy.start()


def wait_blocks(ref, send_sem, recv_sem, peer, incoming):
    copy = pltpu.make_async_remote_copy(
        src_ref=ref, dst_ref=ref, send_sem=send_sem, recv_sem=recv_sem, device_id={"row": peer}, device_id_type=MESH
    )
    if incoming:
        copy.wait_recv()
    else:
        copy.wait_send()


def kernel(
    n,
    total_samples,
    total_rows,
    k_hbm,
    j_hbm,
    pick_hbm,
    count_hbm,
    b_hbm,
    c_hbm,
    w_hbm,
    values_hbm,
    update_hbm,
    scales_ref,
    k_ref,
    j_ref,
    pick_ref,
    count_ref,
    b_ref,
    c_ref,
    w_ref,
    values_ref,
    table_c,
    table_b,
    stage,
    c_out,
    c_in,
    wb,
    wp,
    wk,
    values_out,
    values_in,
    rows_out,
    rows_in,
    g_out,
    g_one,
    g_mid,
    g_two,
    g_sum,
    g_all,
    s_out,
    s_in,
    update_ref,
    local,
    c_recv,
    c_send,
    v_send,
    v_recv,
    r_send,
    r_recv,
    s_send,
    s_recv,
    small_send,
    small_recv,
):
    me = lax.axis_index("row")
    rank = b_ref.shape[0]
    depth_c, depth_b = c_ref.shape[1], b_ref.shape[1]
    per = k_ref.shape[0] // n
    half = per // 2
    side = 8
    assert depth_c & (depth_c - 1) == 0 and depth_b & (depth_b - 1) == 0
    ring, seat = me // side, me % side
    lane = lax.broadcasted_iota(jnp.int32, (1, 128), 1)
    left = lane < rank

    barrier = pltpu.get_barrier_semaphore()
    home = (me // 2) * 2

    def greet_chip(offset):
        chip = lax.rem(home + offset, n)
        for core in range(2):
            pl.semaphore_signal(barrier, inc=1, device_id={"row": chip + core}, device_id_type=MESH)

    def greet(i, _):
        greet_chip(n // 2 - 2 * i)
        greet_chip(n // 2 + 2 * i)
        return 0

    loads = [
        pltpu.make_async_copy(src, dst, local.at[i])
        for i, (src, dst) in enumerate(
            (
                (count_hbm, count_ref),
                (values_hbm, values_ref),
                (c_hbm, c_ref),
                (k_hbm, k_ref),
                (b_hbm, b_ref),
                (j_hbm, j_ref),
                (w_hbm, w_ref),
                (pick_hbm, pick_ref),
            )
        )
    ]
    for copy in loads:
        copy.start()
    greet_chip(n // 2)
    lax.fori_loop(1, n // 4, greet, 0)
    pl.semaphore_signal(barrier, inc=1, device_id={"row": home + 1 - me % 2}, device_id_type=MESH)

    def fill(table, ref):
        def chunk(i, _):
            at = pl.multiple_of(i * 128, 128)
            part = ref[:, pl.ds(at, 128)].astype(F32).T
            table[pl.ds(at, 128), :] = jnp.concatenate([part, part], axis=1)
            return 0

        lax.fori_loop(0, ref.shape[1] // 128, chunk, 0)

    def rows_of(table, index_ref, at, mask):
        for i in range(half):
            first = table[pl.ds(index_ref[at + i] & mask, 1), :]
            second = table[pl.ds(index_ref[at + half + i] & mask, 1), :]
            stage[i : i + 1, :] = jnp.where(left, first, second)
        return stage[...]

    loads[0].wait()
    loads[1].wait()
    counts = count_ref[...]
    live = jnp.sum(jnp.sum(counts.astype(F32), axis=1, keepdims=True), axis=0, keepdims=True)
    counts = jnp.concatenate([counts, counts], axis=1)

    def mask_values(peer):
        turned = pltpu.roll(counts, 128 - peer, 1)
        for part in range(2):
            kept = lane < turned[part * 8 : part * 8 + 8, 0:1]
            values_out[peer, part] = jnp.where(kept, values_ref[peer, part].astype(F32), 0.0).astype(BF16)

    far = [lax.rem(home + n // 2, n), lax.rem(home + n // 2, n) + 1]
    mate = home + 1 - me % 2
    reach = n // 4 - 1

    def peers(dist):
        up = lax.rem(home + 2 * dist, n)
        down = lax.rem(home + n - 2 * dist, n)
        return up, up + 1, down, down + 1

    def by_distance(high, low, act):
        def body(i, _):
            for peer in peers(high - i):
                act(peer)
            return 0

        lax.fori_loop(0, high - low + 1, body, 0)

    def send_value(peer):
        send(values_out.at[peer], values_in.at[me], v_send, v_recv, peer)

    early = reach - 3

    def both(i, _):
        for peer in peers(reach - i):
            mask_values(peer)
        for peer in peers(reach - i + 1):
            send_value(peer)
        return 0

    mask_values(me)
    values_in[me] = values_out[me]
    for peer in far:
        mask_values(peer)
    loads[2].wait()
    fill(table_c, c_ref)
    pl.semaphore_wait(barrier, n - 1)
    for peer in peers(reach):
        mask_values(peer)
    for peer in far:
        send_value(peer)
    lax.fori_loop(1, reach - early + 1, both, 0)
    for peer in peers(early):
        send_value(peer)

    loads[3].wait()

    def gather_c(i, _):
        peer = jnp.where(i == n - 1, me, partner(i, me, n, 1))
        c_out[peer] = rows_of(table_c, k_ref, peer * per, depth_c - 1).astype(BF16)
        return 0

    lax.fori_loop(0, n, gather_c, 0)

    def send_c(peer):
        send(c_out.at[peer], c_in.at[me], c_send, c_recv.at[me], peer)

    for peer in far:
        send_c(peer)
    by_distance(reach, 1, send_c)
    send_c(mate)
    by_distance(early - 1, 1, mask_values)
    mask_values(mate)

    for copy in loads[4:]:
        copy.wait()
    fill(table_b, b_ref)

    def weigh(i, _):
        turned = w_ref[pl.ds(pl.multiple_of(i * 8, 8), 8), :].T
        for j in range(8):
            wp[i * 8 + j] = jnp.where(left, turned[:half, j : j + 1], turned[half:, j : j + 1])
        return 0

    lax.fori_loop(0, n // 8, weigh, 0)

    def gather_b(e, _):
        wb[e] = rows_of(table_b, j_ref, e * per, depth_b - 1) * wp[e]
        return 0

    lax.fori_loop(0, n, gather_b, 0)

    def use(e, c_rows, gram):
        sketch = wb[e] * c_rows.astype(F32)
        weighted = wp[e] * sketch
        turned = pltpu.roll(weighted, rank, 1)
        at = pl.multiple_of(e * per, 128)
        wk[pl.ds(at, half), :] = jnp.where(left, weighted, turned)
        wk[pl.ds(at + half, half), :] = jnp.where(left, turned, weighted)
        return gram + lax.dot_general(
            sketch, sketch, (((0,), (0,)), ((), ())), precision=HIGHEST, preferred_element_type=F32
        )

    gram = use(me, c_out[me], jnp.zeros((128, 128), F32))

    def take(i, gram):
        e = partner(i, me, n, -1)
        wait_blocks(c_in.at[e], c_send, c_recv.at[e], e, True)
        return use(e, c_in[e], gram)

    gram = lax.fori_loop(0, n - 1, take, gram)

    eye = lax.broadcasted_iota(jnp.int32, (rank, 128), 0) == lax.broadcasted_iota(jnp.int32, (rank, 128), 1)
    square = gram[:rank, :rank] + gram[rank:, rank:]
    system = square * (1.0 / total_samples) + jnp.where(eye[:, :rank], live * (0.05 / total_rows), 0.0)
    packed = jnp.concatenate([system[: rank // 2], system[rank // 2 :]], axis=1)
    lines = packed.shape[0] // side
    for i in range(side):
        g_out[i] = packed[i * lines : (i + 1) * lines]
    g_one[seat] = g_out[seat]

    def spread(kind, src_of, dst, peer_of, own):
        for j in range(1, side):
            peer, index = peer_of(j)
            send(src_of(index), dst.at[own], small_send.at[kind, index], small_recv.at[kind, own], peer)

    def collect(kind, dst, peer_of):
        for j in range(1, side):
            peer, index = peer_of(j)
            wait_blocks(dst.at[index], small_send.at[kind, index], small_recv.at[kind, index], peer, True)

    def in_ring(j):
        index = lax.rem(seat + j, side)
        return ring * side + index, index

    def across(j):
        index = lax.rem(ring + j, side)
        return index * side + seat, index

    def total_of(ref):
        total = ref[0]
        for i in range(1, side):
            total = total + ref[i]
        return total

    spread(0, lambda i: g_out.at[i], g_one, in_ring, seat)
    middle = early - 2
    by_distance(early - 1, middle, send_value)

    def pick(q, _):
        for i in range(8):
            first = wk[pl.ds(pick_ref[i, q], 1), :]
            second = wk[pl.ds(pick_ref[8 + i, q], 1), :]
            stage[i : i + 1, :] = jnp.where(left, first, second)
        rows_out[q] = stage[0:8, :].astype(BF16)
        return 0

    lax.fori_loop(0, n, pick, 0)

    collect(0, g_one, in_ring)
    total = total_of(g_one)
    g_mid[...] = total
    g_two[ring] = total
    spread(1, lambda i: g_mid, g_two, across, ring)

    def send_rows(peer):
        send(rows_out.at[peer], rows_in.at[me], r_send, r_recv, peer)

    by_distance(middle - 1, 1, send_value)
    send_value(mate)
    for peer in far:
        send_rows(peer)
    by_distance(reach, reach, send_rows)
    rows_in[me] = rows_out[me]

    collect(1, g_two, across)
    total = total_of(g_two)
    g_sum[...] = total
    g_all[seat] = total
    spread(2, lambda i: g_sum, g_all, in_ring, seat)
    by_distance(reach - 1, 1, send_rows)
    send_rows(mate)
    collect(2, g_all, in_ring)
    packed = jnp.concatenate([g_all[i] for i in range(side)], axis=0)
    matrix = jnp.concatenate([packed, pltpu.roll(packed, rank, 1)], axis=0)
    matrix = jnp.where(left, matrix, pltpu.roll(matrix, rank, 1))

    row_at = lax.broadcasted_iota(jnp.int32, (rank, 1), 0)
    lane_at = lax.rem(lane, rank)

    def eliminate(_, m):
        for i in range(0, 8, 2):
            one = jnp.broadcast_to(m[:, i : i + 1], m.shape)
            two = jnp.broadcast_to(m[:, i + 1 : i + 2], m.shape)
            a, b = one[i : i + 1, :], one[i + 1 : i + 2, :]
            c, d = two[i : i + 1, :], two[i + 1 : i + 2, :]
            scale = 1.0 / (a * d - b * c)
            upper = jnp.where(lane_at == i, 1.0, jnp.where(lane_at == i + 1, 0.0, m[i : i + 1, :]))
            lower = jnp.where(lane_at == i, 0.0, jnp.where(lane_at == i + 1, 1.0, m[i + 1 : i + 2, :]))
            first = (d * scale) * upper - (c * scale) * lower
            second = (a * scale) * lower - (b * scale) * upper
            rest = jnp.where(lane_at // 2 == i // 2, 0.0, m) - one * first - two * second
            m = jnp.where(row_at == i, first, jnp.where(row_at == i + 1, second, rest))
        m = pltpu.roll(m, 120, 1)
        return jnp.concatenate([m[8:], m[:8]], axis=0)

    inverse = lax.fori_loop(0, rank // 8, eliminate, matrix)[:, :rank]

    rest = pl.ds(0, n - 1)
    wait_blocks(values_in.at[rest], v_send, v_recv, mate, True)
    wait_blocks(rows_in.at[rest], r_send, r_recv, mate, True)

    rows = rows_in[...].astype(F32).reshape(n * 8, 128)
    low = values_in[:, 0].astype(F32).reshape(n * 8, 128).astype(BF16)
    high = values_in[:, 1].astype(F32).reshape(n * 8, 128).astype(BF16)
    slot = lax.rem(lax.broadcasted_iota(jnp.int32, (n * 8, 1), 0), 8)

    def mixed(mask, values):
        return lax.dot_general(
            jnp.where(mask, rows, 0.0).astype(BF16), values, (((0,), (0,)), ((), ())), preferred_element_type=F32
        )

    gathered = [
        mixed(slot < 4, low)[:rank],
        mixed(slot >= 4, low)[:rank],
        mixed(slot < 4, high)[rank:],
        mixed(slot >= 4, high)[rank:],
    ]
    squares = jnp.zeros((rank, 128), F32)
    for t, g in enumerate(gathered):
        u = lax.dot_general(inverse, g, (((1,), (0,)), ((), ())), precision=HIGHEST, preferred_element_type=F32)
        update_ref[:, t * 128 : (t + 1) * 128] = u
        squares = squares + u * u
    own = jnp.sum(squares, axis=1, keepdims=True)
    own = jnp.sum(jnp.where(eye, own, 0.0), axis=0, keepdims=True)
    s_out[...] = own
    s_in[me] = own

    def send_sums(peer):
        send(s_out, s_in.at[me], s_send, s_recv, peer)

    for peer in far:
        send_sums(peer)
    by_distance(reach, 1, send_sums)
    send_sums(mate)
    leave = pltpu.make_async_copy(update_ref, update_hbm, local.at[len(loads)])
    leave.start()
    wait_blocks(values_out.at[rest], v_send, v_recv, mate, False)
    wait_blocks(c_out.at[rest], c_send, c_recv.at[me], mate, False)
    wait_blocks(rows_out.at[rest], r_send, r_recv, mate, False)
    for kind, ref, peer_of in ((0, g_out.at[0], in_ring), (1, g_mid, across), (2, g_sum, in_ring)):
        for j in range(1, side):
            peer, index = peer_of(j)
            wait_blocks(ref, small_send.at[kind, index], small_recv.at[kind, index], peer, False)
    leave.wait()
    wait_blocks(s_in.at[rest], s_send, s_recv, mate, False)
    wait_blocks(s_in.at[rest], s_send, s_recv, mate, True)
    total = jnp.sum(s_in[...], axis=0)
    scales_ref[...] = jnp.sqrt(total / total_rows + 1e-06)


def solution(mesh):
    n = mesh.shape["row"]

    def shards(
        factor_b, factor_c, sample_j, sample_k, sample_weight, block_values, block_sample, block_count
    ):
        rank = factor_b.shape[0]
        samples = sample_j.shape[0]
        _, _, tiles, slots, width = block_values.shape
        values = block_values.reshape(n, 2, tiles * slots // 2, width)
        counts = block_count[0].transpose(1, 2, 0).reshape(tiles * slots, n)
        picks = block_sample[0].transpose(1, 2, 0).reshape(tiles * slots, n)
        weights = sample_weight.reshape(n, -1)
        vmem = pl.BlockSpec(memory_space=pltpu.VMEM)
        anywhere = pl.BlockSpec(memory_space=pl.ANY)
        half = samples // n // 2
        update, scales = pl.pallas_call(
            functools.partial(kernel, n, samples * n, tiles * width * n),
            out_shape=(
                jax.ShapeDtypeStruct((rank, tiles * width), F32),
                jax.ShapeDtypeStruct((1, 128), F32),
            ),
            in_specs=[anywhere] * 8,
            out_specs=(anywhere, vmem),
            scratch_shapes=[
                pltpu.SMEM((samples,), jnp.int32),
                pltpu.SMEM((samples,), jnp.int32),
                pltpu.SMEM(picks.shape, jnp.int32),
                pltpu.VMEM(counts.shape, jnp.int32),
                pltpu.VMEM(factor_b.shape, BF16),
                pltpu.VMEM(factor_c.shape, BF16),
                pltpu.VMEM(weights.shape, F32),
                pltpu.VMEM(values.shape, BF16),
                pltpu.VMEM((factor_c.shape[1], 128), F32),
                pltpu.VMEM((factor_b.shape[1], 128), F32),
                pltpu.VMEM((half, 128), F32),
                pltpu.VMEM((n, half, 128), BF16),
                pltpu.VMEM((n, half, 128), BF16),
                pltpu.VMEM((n, half, 128), F32),
                pltpu.VMEM((n, half, 128), F32),
                pltpu.VMEM((samples, 128), F32),
                pltpu.VMEM(values.shape, BF16),
                pltpu.VMEM(values.shape, BF16),
                pltpu.VMEM((n, 8, 128), BF16),
                pltpu.VMEM((n, 8, 128), BF16),
                pltpu.VMEM((8, 4, 128), F32),
                pltpu.VMEM((8, 4, 128), F32),
                pltpu.VMEM((4, 128), F32),
                pltpu.VMEM((8, 4, 128), F32),
                pltpu.VMEM((4, 128), F32),
                pltpu.VMEM((8, 4, 128), F32),
                pltpu.VMEM((1, 128), F32),
                pltpu.VMEM((n, 1, 128), F32),
                pltpu.VMEM((rank, tiles * width), F32),
                pltpu.SemaphoreType.DMA((9,)),
                pltpu.SemaphoreType.DMA((n,)),
            ]
            + [pltpu.SemaphoreType.DMA(())] * 7
            + [pltpu.SemaphoreType.DMA((3, 8))] * 2,
            compiler_params=pltpu.CompilerParams(collective_id=0, has_side_effects=True),
            name="step",
        )(
            sample_k.reshape(-1),
            sample_j,
            picks,
            counts,
            factor_b,
            factor_c,
            weights,
            values,
        )
        scales = scales[0, :rank]
        return (update / scales[:, None]).astype(BF16), scales

    return jax.shard_map(
        shards,
        mesh=mesh,
        in_specs=(
            P(None, GROUPS_ROW),
            P(None, GROUPS_ROW),
            P(GROUPS_ROW),
            P(None, GROUPS_ROW, None),
            P(GROUPS_ROW),
            P(GROUPS_ROW, None, None, None, None),
            P(GROUPS_ROW, None, None, None),
            P(GROUPS_ROW, None, None, None),
        ),
        out_specs=(P(None, GROUPS_ROW), P("groups")),
        check_vma=False,
    )
```

```python
import functools

import jax
import jax.numpy as jnp
from jax import lax
from jax.experimental import pallas as pl
from jax.experimental.pallas import tpu as pltpu
from jax.sharding import PartitionSpec as P

MESH = pl.DeviceIdType.MESH
GROUPS_ROW = ("groups", "row")
HIGHEST = lax.Precision.HIGHEST
F32 = jnp.float32
BF16 = jnp.bfloat16


def partner(step, me, n, sign):
    chips = n // 2
    z, core = me // 2, me % 2
    rest = step - 2
    dist = jnp.where(step < 2, chips // 2, chips // 2 - 1 - rest // 4)
    way = jnp.where(step < 2, 1, 1 - 2 * ((rest // 2) % 2)) * sign
    other = jnp.where(step < 2, step, rest % 2)
    other = jnp.where(step == n - 2, 1 - core, other)
    return lax.rem(z + dist * way + chips, chips) * 2 + other


def send(src, dst, send_sem, recv_sem, peer):
    copy = pltpu.make_async_remote_copy(
        src_ref=src,
        dst_ref=dst,
        send_sem=send_sem,
        recv_sem=recv_sem,
        device_id={"row": peer},
        device_id_type=MESH,
    )
    copy.start()


def wait_blocks(ref, send_sem, recv_sem, peer, incoming):
    copy = pltpu.make_async_remote_copy(
        src_ref=ref, dst_ref=ref, send_sem=send_sem, recv_sem=recv_sem, device_id={"row": peer}, device_id_type=MESH
    )
    if incoming:
        copy.wait_recv()
    else:
        copy.wait_send()


def kernel(
    n,
    total_samples,
    total_rows,
    k_hbm,
    j_hbm,
    pick_hbm,
    count_hbm,
    b_hbm,
    c_hbm,
    w_hbm,
    values_hbm,
    update_hbm,
    scales_ref,
    k_ref,
    j_ref,
    pick_ref,
    count_ref,
    b_ref,
    c_ref,
    w_ref,
    values_ref,
    table_c,
    table_b,
    stage,
    c_out,
    c_in,
    wb,
    wp,
    wk,
    block_out,
    block_in,
    g_out,
    g_one,
    g_mid,
    g_two,
    g_sum,
    g_all,
    s_out,
    s_in,
    update_ref,
    local,
    c_recv,
    c_send,
    b_send,
    b_recv,
    s_send,
    s_recv,
    small_send,
    small_recv,
):
    me = lax.axis_index("row")
    rank = b_ref.shape[0]
    depth_c, depth_b = c_ref.shape[1], b_ref.shape[1]
    per = k_ref.shape[0] // n
    half = per // 2
    side = 8
    assert depth_c & (depth_c - 1) == 0 and depth_b & (depth_b - 1) == 0
    ring, seat = me // side, me % side
    lane = lax.broadcasted_iota(jnp.int32, (1, 128), 1)
    left = lane < rank

    barrier = pltpu.get_barrier_semaphore()
    home = (me // 2) * 2

    def greet_chip(offset):
        chip = lax.rem(home + offset, n)
        for core in range(2):
            pl.semaphore_signal(barrier, inc=1, device_id={"row": chip + core}, device_id_type=MESH)

    def greet(i, _):
        greet_chip(n // 2 - 2 * i)
        greet_chip(n // 2 + 2 * i)
        return 0

    loads = [
        pltpu.make_async_copy(src, dst, local.at[i])
        for i, (src, dst) in enumerate(
            (
                (count_hbm, count_ref),
                (values_hbm, values_ref),
                (c_hbm, c_ref),
                (k_hbm, k_ref),
                (b_hbm, b_ref),
                (j_hbm, j_ref),
                (w_hbm, w_ref),
                (pick_hbm, pick_ref),
            )
        )
    ]
    for copy in loads:
        copy.start()
    greet_chip(n // 2)
    lax.fori_loop(1, n // 4, greet, 0)
    pl.semaphore_signal(barrier, inc=1, device_id={"row": home + 1 - me % 2}, device_id_type=MESH)

    def fill(table, ref):
        def chunk(i, _):
            for j in range(4):
                at = pl.multiple_of(i * 512 + j * 128, 128)
                part = ref[:, pl.ds(at, 128)].astype(F32)
                table[pl.ds(at, 128), :] = jnp.concatenate([part, part], axis=0).T
            return 0

        lax.fori_loop(0, ref.shape[1] // 512, chunk, 0)

    def rows_of(table, index_ref, at, mask):
        for i in range(half):
            first = table[pl.ds(index_ref[at + i] & mask, 1), :]
            second = table[pl.ds(index_ref[at + half + i] & mask, 1), :]
            stage[i : i + 1, :] = jnp.where(left, first, second)
        return stage[...]

    loads[0].wait()
    loads[1].wait()
    counts = count_ref[...]
    live = jnp.sum(jnp.sum(counts.astype(F32), axis=1, keepdims=True), axis=0, keepdims=True)
    counts = jnp.concatenate([counts, counts], axis=1)

    def mask_values(peer):
        turned = pltpu.roll(counts, 128 - peer, 1)
        for part in range(2):
            kept = lane < turned[part * 8 : part * 8 + 8, 0:1]
            block_out[peer, part] = jnp.where(kept, values_ref[peer, part].astype(F32), 0.0).astype(BF16)

    far = [lax.rem(home + n // 2, n), lax.rem(home + n // 2, n) + 1]
    mate = home + 1 - me % 2
    reach = n // 4 - 1

    def peers(dist):
        up = lax.rem(home + 2 * dist, n)
        down = lax.rem(home + n - 2 * dist, n)
        return up, up + 1, down, down + 1

    def by_distance(high, low, act):
        def body(i, _):
            for peer in peers(high - i):
                act(peer)
            return 0

        lax.fori_loop(0, high - low + 1, body, 0)

    def send_value(peer):
        pair = pl.ds(0, 2)
        send(block_out.at[peer, pair], block_in.at[me, pair], b_send, b_recv, peer)

    def send_rows(peer):
        send(block_out.at[peer, 2], block_in.at[me, 2], b_send, b_recv, peer)

    def send_block(peer):
        send(block_out.at[peer], block_in.at[me], b_send, b_recv, peer)

    early = reach - 5

    def both(i, _):
        for peer in peers(reach - i):
            mask_values(peer)
        for peer in peers(reach - i + 1):
            send_value(peer)
        return 0

    mask_values(me)
    for peer in far:
        mask_values(peer)
    pl.semaphore_wait(barrier, n - 1)
    for peer in peers(reach):
        mask_values(peer)
    for peer in far:
        send_value(peer)
    lax.fori_loop(1, reach - early + 1, both, 0)
    for peer in peers(early):
        send_value(peer)

    loads[2].wait()
    fill(table_c, c_ref)
    loads[3].wait()

    def gather_c(peer):
        c_out[peer] = rows_of(table_c, k_ref, peer * per, depth_c - 1).astype(BF16)

    def send_c(peer):
        send(c_out.at[peer], c_in.at[me], c_send, c_recv.at[me], peer)

    def gather_and_send(i, _):
        gather_c(partner(i, me, n, 1))
        send_c(partner(i - 1, me, n, 1))
        return 0

    gather_c(far[0])
    lax.fori_loop(1, n - 1, gather_and_send, 0)
    gather_c(me)
    send_c(mate)
    by_distance(early - 1, 1, mask_values)
    mask_values(mate)

    for copy in loads[4:]:
        copy.wait()
    fill(table_b, b_ref)

    def weigh(i, _):
        turned = w_ref[pl.ds(pl.multiple_of(i * 8, 8), 8), :].T
        for j in range(8):
            wp[i * 8 + j] = jnp.where(left, turned[:half, j : j + 1], turned[half:, j : j + 1])
        return 0

    lax.fori_loop(0, n // 8, weigh, 0)

    def gather_b(e, _):
        wb[e] = rows_of(table_b, j_ref, e * per, depth_b - 1) * wp[e]
        return 0

    lax.fori_loop(0, n, gather_b, 0)

    def use(e, c_rows, gram):
        sketch = wb[e] * c_rows.astype(F32)
        weighted = wp[e] * sketch
        turned = pltpu.roll(weighted, rank, 1)
        at = pl.multiple_of(e * per, 128)
        wk[pl.ds(at, half), :] = jnp.where(left, weighted, turned)
        wk[pl.ds(at + half, half), :] = jnp.where(left, turned, weighted)
        return gram + lax.dot_general(
            sketch, sketch, (((0,), (0,)), ((), ())), precision=HIGHEST, preferred_element_type=F32
        )

    gram = use(me, c_out[me], jnp.zeros((128, 128), F32))

    def take(i, gram):
        e = partner(i, me, n, -1)
        wait_blocks(c_in.at[e], c_send, c_recv.at[e], e, True)
        return use(e, c_in[e], gram)

    gram = lax.fori_loop(0, n - 1, take, gram)

    eye = lax.broadcasted_iota(jnp.int32, (rank, 128), 0) == lax.broadcasted_iota(jnp.int32, (rank, 128), 1)
    square = gram[:rank, :rank] + gram[rank:, rank:]
    system = square * (1.0 / total_samples) + jnp.where(eye[:, :rank], live * (0.05 / total_rows), 0.0)
    packed = jnp.concatenate([system[: rank // 2], system[rank // 2 :]], axis=1)
    lines = packed.shape[0] // side
    for i in range(side):
        g_out[i] = packed[i * lines : (i + 1) * lines]
    g_one[seat] = g_out[seat]

    def spread(kind, src_of, dst, peer_of, own):
        for j in range(1, side):
            peer, index = peer_of(j)
            send(src_of(index), dst.at[own], small_send.at[kind, index], small_recv.at[kind, own], peer)

    def collect(kind, dst, peer_of):
        for j in range(1, side):
            peer, index = peer_of(j)
            wait_blocks(dst.at[index], small_send.at[kind, index], small_recv.at[kind, index], peer, True)

    def in_ring(j):
        index = lax.rem(seat + j, side)
        return ring * side + index, index

    def across(j):
        index = lax.rem(ring + j, side)
        return index * side + seat, index

    def total_of(ref):
        total = ref[0]
        for i in range(1, side):
            total = total + ref[i]
        return total

    spread(0, lambda i: g_out.at[i], g_one, in_ring, seat)
    def pick(q, _):
        for i in range(8):
            first = wk[pl.ds(pick_ref[i, q], 1), :]
            second = wk[pl.ds(pick_ref[8 + i, q], 1), :]
            stage[i : i + 1, :] = jnp.where(left, first, second)
        block_out[q, 2] = stage[0:8, :].astype(BF16)
        return 0

    lax.fori_loop(0, n, pick, 0)
    for peer in far:
        send_rows(peer)
    by_distance(reach, reach, send_rows)
    block_in[me] = block_out[me]

    collect(0, g_one, in_ring)
    total = total_of(g_one)
    g_mid[...] = total
    g_two[ring] = total
    spread(1, lambda i: g_mid, g_two, across, ring)

    middle = early - 3
    by_distance(reach - 1, early, send_rows)
    by_distance(early - 1, middle, send_block)
    collect(1, g_two, across)
    total = total_of(g_two)
    g_sum[...] = total
    g_all[seat] = total
    spread(2, lambda i: g_sum, g_all, in_ring, seat)
    by_distance(middle - 1, 1, send_block)
    send_block(mate)
    collect(2, g_all, in_ring)
    packed = jnp.concatenate([g_all[i] for i in range(side)], axis=0)
    matrix = jnp.concatenate([packed, pltpu.roll(packed, rank, 1)], axis=0)
    matrix = jnp.where(left, matrix, pltpu.roll(matrix, rank, 1))

    row_at = lax.broadcasted_iota(jnp.int32, (rank, 1), 0)
    lane_at = lax.rem(lane, rank)

    def eliminate(_, m):
        for i in range(0, 8, 2):
            one = jnp.broadcast_to(m[:, i : i + 1], m.shape)
            two = jnp.broadcast_to(m[:, i + 1 : i + 2], m.shape)
            a, b = one[i : i + 1, :], one[i + 1 : i + 2, :]
            c, d = two[i : i + 1, :], two[i + 1 : i + 2, :]
            scale = 1.0 / (a * d - b * c)
            upper = jnp.where(lane_at == i, 1.0, jnp.where(lane_at == i + 1, 0.0, m[i : i + 1, :]))
            lower = jnp.where(lane_at == i, 0.0, jnp.where(lane_at == i + 1, 1.0, m[i + 1 : i + 2, :]))
            first = (d * scale) * upper - (c * scale) * lower
            second = (a * scale) * lower - (b * scale) * upper
            rest = jnp.where(lane_at // 2 == i // 2, 0.0, m) - one * first - two * second
            m = jnp.where(row_at == i, first, jnp.where(row_at == i + 1, second, rest))
        m = pltpu.roll(m, 120, 1)
        return jnp.concatenate([m[8:], m[:8]], axis=0)

    inverse = lax.fori_loop(0, rank // 8, eliminate, matrix)[:, :rank]

    rest = pl.ds(0, n - 1)
    wait_blocks(block_in.at[rest], b_send, b_recv, mate, True)

    rows = block_in[:, 2].astype(F32).reshape(n * 8, 128)
    low = block_in[:, 0].astype(F32).reshape(n * 8, 128).astype(BF16)
    high = block_in[:, 1].astype(F32).reshape(n * 8, 128).astype(BF16)
    slot = lax.rem(lax.broadcasted_iota(jnp.int32, (n * 8, 1), 0), 8)

    def mixed(mask, values):
        return lax.dot_general(
            jnp.where(mask, rows, 0.0).astype(BF16), values, (((0,), (0,)), ((), ())), preferred_element_type=F32
        )

    gathered = [
        mixed(slot < 4, low)[:rank],
        mixed(slot >= 4, low)[:rank],
        mixed(slot < 4, high)[rank:],
        mixed(slot >= 4, high)[rank:],
    ]
    squares = jnp.zeros((rank, 128), F32)
    for t, g in enumerate(gathered):
        u = lax.dot_general(inverse, g, (((1,), (0,)), ((), ())), precision=HIGHEST, preferred_element_type=F32)
        update_ref[:, t * 128 : (t + 1) * 128] = u
        squares = squares + u * u
    own = jnp.sum(squares, axis=1, keepdims=True)
    own = jnp.sum(jnp.where(eye, own, 0.0), axis=0, keepdims=True)
    s_out[...] = own
    s_in[me] = own

    def send_sums(peer):
        send(s_out, s_in.at[me], s_send, s_recv, peer)

    for peer in far:
        send_sums(peer)
    by_distance(reach, 1, send_sums)
    send_sums(mate)
    leave = pltpu.make_async_copy(update_ref, update_hbm, local.at[len(loads)])
    leave.start()
    wait_blocks(block_out.at[rest], b_send, b_recv, mate, False)
    wait_blocks(c_out.at[rest], c_send, c_recv.at[me], mate, False)
    for kind, ref, peer_of in ((0, g_out.at[0], in_ring), (1, g_mid, across), (2, g_sum, in_ring)):
        for j in range(1, side):
            peer, index = peer_of(j)
            wait_blocks(ref, small_send.at[kind, index], small_recv.at[kind, index], peer, False)
    leave.wait()
    wait_blocks(s_in.at[rest], s_send, s_recv, mate, False)
    wait_blocks(s_in.at[rest], s_send, s_recv, mate, True)
    total = jnp.sum(s_in[...], axis=0)
    scales_ref[...] = jnp.sqrt(total / total_rows + 1e-06)


def solution(mesh):
    n = mesh.shape["row"]

    def shards(
        factor_b, factor_c, sample_j, sample_k, sample_weight, block_values, block_sample, block_count
    ):
        rank = factor_b.shape[0]
        samples = sample_j.shape[0]
        _, _, tiles, slots, width = block_values.shape
        values = block_values.reshape(n, 2, tiles * slots // 2, width)
        counts = block_count[0].transpose(1, 2, 0).reshape(tiles * slots, n)
        picks = block_sample[0].transpose(1, 2, 0).reshape(tiles * slots, n)
        weights = sample_weight.reshape(n, -1)
        vmem = pl.BlockSpec(memory_space=pltpu.VMEM)
        anywhere = pl.BlockSpec(memory_space=pl.ANY)
        half = samples // n // 2
        update, scales = pl.pallas_call(
            functools.partial(kernel, n, samples * n, tiles * width * n),
            out_shape=(
                jax.ShapeDtypeStruct((rank, tiles * width), F32),
                jax.ShapeDtypeStruct((1, 128), F32),
            ),
            in_specs=[anywhere] * 8,
            out_specs=(anywhere, vmem),
            scratch_shapes=[
                pltpu.SMEM((samples,), jnp.int32),
                pltpu.SMEM((samples,), jnp.int32),
                pltpu.SMEM(picks.shape, jnp.int32),
                pltpu.VMEM(counts.shape, jnp.int32),
                pltpu.VMEM(factor_b.shape, BF16),
                pltpu.VMEM(factor_c.shape, BF16),
                pltpu.VMEM(weights.shape, F32),
                pltpu.VMEM(values.shape, BF16),
                pltpu.VMEM((factor_c.shape[1], 128), F32),
                pltpu.VMEM((factor_b.shape[1], 128), F32),
                pltpu.VMEM((half, 128), F32),
                pltpu.VMEM((n, half, 128), BF16),
                pltpu.VMEM((n, half, 128), BF16),
                pltpu.VMEM((n, half, 128), F32),
                pltpu.VMEM((n, half, 128), F32),
                pltpu.VMEM((samples, 128), F32),
                pltpu.VMEM((n, 3, 8, 128), BF16),
                pltpu.VMEM((n, 3, 8, 128), BF16),
                pltpu.VMEM((8, 4, 128), F32),
                pltpu.VMEM((8, 4, 128), F32),
                pltpu.VMEM((4, 128), F32),
                pltpu.VMEM((8, 4, 128), F32),
                pltpu.VMEM((4, 128), F32),
                pltpu.VMEM((8, 4, 128), F32),
                pltpu.VMEM((1, 128), F32),
                pltpu.VMEM((n, 1, 128), F32),
                pltpu.VMEM((rank, tiles * width), F32),
                pltpu.SemaphoreType.DMA((9,)),
                pltpu.SemaphoreType.DMA((n,)),
            ]
            + [pltpu.SemaphoreType.DMA(())] * 5
            + [pltpu.SemaphoreType.DMA((3, 8))] * 2,
            compiler_params=pltpu.CompilerParams(collective_id=0, has_side_effects=True),
            name="step",
        )(
            sample_k.reshape(-1),
            sample_j,
            picks,
            counts,
            factor_b,
            factor_c,
            weights,
            values,
        )
        scales = scales[0, :rank]
        return (update / scales[:, None]).astype(BF16), scales

    return jax.shard_map(
        shards,
        mesh=mesh,
        in_specs=(
            P(None, GROUPS_ROW),
            P(None, GROUPS_ROW),
            P(GROUPS_ROW),
            P(None, GROUPS_ROW, None),
            P(GROUPS_ROW),
            P(GROUPS_ROW, None, None, None, None),
            P(GROUPS_ROW, None, None, None),
            P(GROUPS_ROW, None, None, None),
        ),
        out_specs=(P(None, GROUPS_ROW), P("groups")),
        check_vma=False,
    )
```

```python
import functools

import jax
import jax.numpy as jnp
from jax import lax
from jax.experimental import pallas as pl
from jax.experimental.pallas import tpu as pltpu
from jax.sharding import PartitionSpec as P

MESH = pl.DeviceIdType.MESH
GROUPS_ROW = ("groups", "row")
HIGHEST = lax.Precision.HIGHEST
F32 = jnp.float32
BF16 = jnp.bfloat16


def partner(step, me, n, sign):
    chips = n // 2
    z, core = me // 2, me % 2
    rest = step - 2
    dist = jnp.where(step < 2, chips // 2, chips // 2 - 1 - rest // 4)
    way = jnp.where(step < 2, 1, 1 - 2 * ((rest // 2) % 2)) * sign
    other = jnp.where(step < 2, step, rest % 2)
    other = jnp.where(step == n - 2, 1 - core, other)
    return lax.rem(z + dist * way + chips, chips) * 2 + other


def send(src, dst, send_sem, recv_sem, peer):
    copy = pltpu.make_async_remote_copy(
        src_ref=src,
        dst_ref=dst,
        send_sem=send_sem,
        recv_sem=recv_sem,
        device_id={"row": peer},
        device_id_type=MESH,
    )
    copy.start()


def wait_blocks(ref, send_sem, recv_sem, peer, incoming):
    copy = pltpu.make_async_remote_copy(
        src_ref=ref, dst_ref=ref, send_sem=send_sem, recv_sem=recv_sem, device_id={"row": peer}, device_id_type=MESH
    )
    if incoming:
        copy.wait_recv()
    else:
        copy.wait_send()


def kernel(
    n,
    total_samples,
    total_rows,
    k_hbm,
    j_hbm,
    pick_hbm,
    count_hbm,
    b_hbm,
    c_hbm,
    w_hbm,
    values_hbm,
    update_hbm,
    scales_ref,
    k_ref,
    j_ref,
    pick_ref,
    count_ref,
    b_ref,
    c_ref,
    w_ref,
    values_ref,
    table_c,
    table_b,
    stage,
    c_out,
    c_in,
    wb,
    wp,
    wk,
    block_out,
    block_in,
    g_out,
    g_one,
    g_mid,
    g_two,
    g_sum,
    g_all,
    s_out,
    s_in,
    update_ref,
    local,
    c_recv,
    c_send,
    b_send,
    b_recv,
    s_send,
    s_recv,
    small_send,
    small_recv,
):
    me = lax.axis_index("row")
    rank = b_ref.shape[0]
    depth_c, depth_b = c_ref.shape[1], b_ref.shape[1]
    per = k_ref.shape[0] // n
    half = per // 2
    side = 8
    assert depth_c & (depth_c - 1) == 0 and depth_b & (depth_b - 1) == 0
    ring, seat = me // side, me % side
    lane = lax.broadcasted_iota(jnp.int32, (1, 128), 1)
    left = lane < rank

    barrier = pltpu.get_barrier_semaphore()
    home = (me // 2) * 2

    def greet_chip(offset):
        chip = lax.rem(home + offset, n)
        for core in range(2):
            pl.semaphore_signal(barrier, inc=1, device_id={"row": chip + core}, device_id_type=MESH)

    def greet(i, _):
        greet_chip(n // 2 - 2 * i)
        greet_chip(n // 2 + 2 * i)
        return 0

    loads = [
        pltpu.make_async_copy(src, dst, local.at[i])
        for i, (src, dst) in enumerate(
            (
                (count_hbm, count_ref),
                (values_hbm, values_ref),
                (c_hbm, c_ref),
                (k_hbm, k_ref),
                (b_hbm, b_ref),
                (j_hbm, j_ref),
                (w_hbm, w_ref),
                (pick_hbm, pick_ref),
            )
        )
    ]
    for copy in loads:
        copy.start()
    greet_chip(n // 2)
    lax.fori_loop(1, n // 4, greet, 0)
    pl.semaphore_signal(barrier, inc=1, device_id={"row": home + 1 - me % 2}, device_id_type=MESH)

    def fill(table, ref):
        def chunk(i, _):
            for j in range(4):
                at = pl.multiple_of(i * 512 + j * 128, 128)
                part = ref[:, pl.ds(at, 128)].astype(F32)
                table[pl.ds(at, 128), :] = jnp.concatenate([part, part], axis=0).T
            return 0

        lax.fori_loop(0, ref.shape[1] // 512, chunk, 0)

    def rows_of(table, index_ref, at, mask):
        for i in range(half):
            first = table[pl.ds(index_ref[at + i] & mask, 1), :]
            second = table[pl.ds(index_ref[at + half + i] & mask, 1), :]
            stage[i : i + 1, :] = jnp.where(left, first, second)
        return stage[...]

    loads[0].wait()
    loads[1].wait()
    counts = count_ref[...]
    live = jnp.sum(jnp.sum(counts.astype(F32), axis=1, keepdims=True), axis=0, keepdims=True)
    counts = jnp.concatenate([counts, counts], axis=1)

    def mask_values(peer):
        turned = pltpu.roll(counts, 128 - peer, 1)
        for part in range(2):
            kept = lane < turned[part * 8 : part * 8 + 8, 0:1]
            block_out[peer, part] = jnp.where(kept, values_ref[peer, part].astype(F32), 0.0).astype(BF16)

    far = [lax.rem(home + n // 2, n), lax.rem(home + n // 2, n) + 1]
    mate = home + 1 - me % 2
    reach = n // 4 - 1

    def peers(dist):
        up = lax.rem(home + 2 * dist, n)
        down = lax.rem(home + n - 2 * dist, n)
        return up, up + 1, down, down + 1

    def by_distance(high, low, act):
        def body(i, _):
            for peer in peers(high - i):
                act(peer)
            return 0

        lax.fori_loop(0, high - low + 1, body, 0)

    def send_value(peer):
        pair = pl.ds(0, 2)
        send(block_out.at[peer, pair], block_in.at[me, pair], b_send, b_recv, peer)

    def send_rows(peer):
        send(block_out.at[peer, 2], block_in.at[me, 2], b_send, b_recv, peer)

    def send_block(peer):
        send(block_out.at[peer], block_in.at[me], b_send, b_recv, peer)

    early = reach - 5

    def both(i, _):
        for peer in peers(reach - i):
            mask_values(peer)
        for peer in peers(reach - i + 1):
            send_value(peer)
        return 0

    mask_values(me)
    for peer in far:
        mask_values(peer)
    pl.semaphore_wait(barrier, n - 1)
    for peer in peers(reach):
        mask_values(peer)
    for peer in far:
        send_value(peer)
    lax.fori_loop(1, reach - early + 1, both, 0)
    for peer in peers(early):
        send_value(peer)

    loads[2].wait()
    fill(table_c, c_ref)
    loads[3].wait()

    def gather_c(peer):
        c_out[peer] = rows_of(table_c, k_ref, peer * per, depth_c - 1).astype(BF16)

    def send_c(peer):
        send(c_out.at[peer], c_in.at[me], c_send, c_recv.at[me], peer)

    def gather_and_send(i, _):
        gather_c(partner(i, me, n, 1))
        send_c(partner(i - 1, me, n, 1))
        return 0

    gather_c(far[0])
    lax.fori_loop(1, n - 1, gather_and_send, 0)
    gather_c(me)
    send_c(mate)
    by_distance(early - 1, 1, mask_values)
    mask_values(mate)

    for copy in loads[4:]:
        copy.wait()
    fill(table_b, b_ref)

    def weigh(i, _):
        turned = w_ref[pl.ds(pl.multiple_of(i * 8, 8), 8), :].T
        for j in range(8):
            wp[i * 8 + j] = jnp.where(left, turned[:half, j : j + 1], turned[half:, j : j + 1])
        return 0

    lax.fori_loop(0, n // 8, weigh, 0)

    def gather_b(e, _):
        wb[e] = rows_of(table_b, j_ref, e * per, depth_b - 1) * wp[e]
        return 0

    lax.fori_loop(0, n, gather_b, 0)

    def use(e, c_rows, gram):
        sketch = wb[e] * c_rows.astype(F32)
        weighted = wp[e] * sketch
        turned = pltpu.roll(weighted, rank, 1)
        at = pl.multiple_of(e * per, 128)
        wk[pl.ds(at, half), :] = jnp.where(left, weighted, turned)
        wk[pl.ds(at + half, half), :] = jnp.where(left, turned, weighted)
        return gram + lax.dot_general(
            sketch, sketch, (((0,), (0,)), ((), ())), precision=HIGHEST, preferred_element_type=F32
        )

    gram = use(me, c_out[me], jnp.zeros((128, 128), F32))

    def take(i, gram):
        e = partner(i, me, n, -1)
        wait_blocks(c_in.at[e], c_send, c_recv.at[e], e, True)
        return use(e, c_in[e], gram)

    gram = lax.fori_loop(0, n - 1, take, gram)

    eye = lax.broadcasted_iota(jnp.int32, (rank, 128), 0) == lax.broadcasted_iota(jnp.int32, (rank, 128), 1)
    square = gram[:rank, :rank] + gram[rank:, rank:]
    system = square * (1.0 / total_samples) + jnp.where(eye[:, :rank], live * (0.05 / total_rows), 0.0)
    packed = jnp.concatenate([system[: rank // 2], system[rank // 2 :]], axis=1)
    lines = packed.shape[0] // side
    for i in range(side):
        g_out[i] = packed[i * lines : (i + 1) * lines]
    g_one[seat] = g_out[seat]

    def spread(kind, src_of, dst, peer_of, own):
        for j in range(1, side):
            peer, index = peer_of(j)
            send(src_of(index), dst.at[own], small_send.at[kind, index], small_recv.at[kind, own], peer)

    def collect(kind, dst, peer_of):
        for j in range(1, side):
            peer, index = peer_of(j)
            wait_blocks(dst.at[index], small_send.at[kind, index], small_recv.at[kind, index], peer, True)

    def in_ring(j):
        index = lax.rem(seat + j, side)
        return ring * side + index, index

    def across(j):
        index = lax.rem(ring + j, side)
        return index * side + seat, index

    def total_of(ref):
        total = ref[0]
        for i in range(1, side):
            total = total + ref[i]
        return total

    spread(0, lambda i: g_out.at[i], g_one, in_ring, seat)
    def pick(q, _):
        for i in range(8):
            first = wk[pl.ds(pick_ref[i, q], 1), :]
            second = wk[pl.ds(pick_ref[8 + i, q], 1), :]
            stage[i : i + 1, :] = jnp.where(left, first, second)
        block_out[q, 2] = stage[0:8, :].astype(BF16)
        return 0

    lax.fori_loop(0, n, pick, 0)
    for peer in far:
        send_rows(peer)
    by_distance(reach, reach, send_rows)
    block_in[me] = block_out[me]

    collect(0, g_one, in_ring)
    total = total_of(g_one)
    g_mid[...] = total
    g_two[ring] = total
    spread(1, lambda i: g_mid, g_two, across, ring)

    middle = early - 3
    by_distance(reach - 1, early, send_rows)
    by_distance(early - 1, middle, send_block)
    collect(1, g_two, across)
    total = total_of(g_two)
    g_sum[...] = total
    g_all[seat] = total
    spread(2, lambda i: g_sum, g_all, in_ring, seat)
    by_distance(middle - 1, 1, send_block)
    send_block(mate)
    collect(2, g_all, in_ring)
    packed = jnp.concatenate([g_all[i] for i in range(side)], axis=0)
    matrix = jnp.concatenate([packed, pltpu.roll(packed, rank, 1)], axis=0)
    matrix = jnp.where(left, matrix, pltpu.roll(matrix, rank, 1))

    row_at = lax.broadcasted_iota(jnp.int32, (rank, 1), 0)
    lane_at = lax.rem(lane, rank)

    def eliminate(_, m):
        for start in range(0, 8, 4):
            columns = [jnp.broadcast_to(m[:, start + t : start + t + 1], m.shape) for t in range(4)]
            for t in range(0, 4, 2):
                i = start + t
                one, two = columns[t], columns[t + 1]
                a, b = one[i : i + 1, :], one[i + 1 : i + 2, :]
                c, d = two[i : i + 1, :], two[i + 1 : i + 2, :]
                scale = 1.0 / (a * d - b * c)
                a, b, c, d = a * scale, b * scale, c * scale, d * scale

                def solved(upper, lower, others):
                    first, second = d * upper - c * lower, a * lower - b * upper
                    rest = others - one * first - two * second
                    return jnp.where(row_at == i, first, jnp.where(row_at == i + 1, second, rest))

                for later in range(t + 2, 4):
                    x = columns[later]
                    columns[later] = solved(x[i : i + 1, :], x[i + 1 : i + 2, :], x)
                upper = jnp.where(lane_at == i, 1.0, jnp.where(lane_at == i + 1, 0.0, m[i : i + 1, :]))
                lower = jnp.where(lane_at == i, 0.0, jnp.where(lane_at == i + 1, 1.0, m[i + 1 : i + 2, :]))
                m = solved(upper, lower, jnp.where(lane_at // 2 == i // 2, 0.0, m))
        m = pltpu.roll(m, 120, 1)
        return jnp.concatenate([m[8:], m[:8]], axis=0)

    inverse = lax.fori_loop(0, rank // 8, eliminate, matrix)[:, :rank]

    rest = pl.ds(0, n - 1)
    wait_blocks(block_in.at[rest], b_send, b_recv, mate, True)

    rows = block_in[:, 2].astype(F32).reshape(n * 8, 128)
    low = block_in[:, 0].astype(F32).reshape(n * 8, 128).astype(BF16)
    high = block_in[:, 1].astype(F32).reshape(n * 8, 128).astype(BF16)
    slot = lax.rem(lax.broadcasted_iota(jnp.int32, (n * 8, 1), 0), 8)

    def mixed(mask, values):
        return lax.dot_general(
            jnp.where(mask, rows, 0.0).astype(BF16), values, (((0,), (0,)), ((), ())), preferred_element_type=F32
        )

    gathered = [
        mixed(slot < 4, low)[:rank],
        mixed(slot >= 4, low)[:rank],
        mixed(slot < 4, high)[rank:],
        mixed(slot >= 4, high)[rank:],
    ]
    squares = jnp.zeros((rank, 128), F32)
    for t, g in enumerate(gathered):
        u = lax.dot_general(inverse, g, (((1,), (0,)), ((), ())), precision=HIGHEST, preferred_element_type=F32)
        update_ref[:, t * 128 : (t + 1) * 128] = u
        squares = squares + u * u
    own = jnp.sum(squares, axis=1, keepdims=True)
    own = jnp.sum(jnp.where(eye, own, 0.0), axis=0, keepdims=True)
    s_out[...] = own
    s_in[me] = own

    def send_sums(peer):
        send(s_out, s_in.at[me], s_send, s_recv, peer)

    for peer in far:
        send_sums(peer)
    by_distance(reach, 1, send_sums)
    send_sums(mate)
    leave = pltpu.make_async_copy(update_ref, update_hbm, local.at[len(loads)])
    leave.start()
    wait_blocks(block_out.at[rest], b_send, b_recv, mate, False)
    wait_blocks(c_out.at[rest], c_send, c_recv.at[me], mate, False)
    for kind, ref, peer_of in ((0, g_out.at[0], in_ring), (1, g_mid, across), (2, g_sum, in_ring)):
        for j in range(1, side):
            peer, index = peer_of(j)
            wait_blocks(ref, small_send.at[kind, index], small_recv.at[kind, index], peer, False)
    leave.wait()
    wait_blocks(s_in.at[rest], s_send, s_recv, mate, False)
    wait_blocks(s_in.at[rest], s_send, s_recv, mate, True)
    total = jnp.sum(s_in[...], axis=0)
    scales_ref[...] = jnp.sqrt(total / total_rows + 1e-06)


def solution(mesh):
    n = mesh.shape["row"]

    def shards(
        factor_b, factor_c, sample_j, sample_k, sample_weight, block_values, block_sample, block_count
    ):
        rank = factor_b.shape[0]
        samples = sample_j.shape[0]
        _, _, tiles, slots, width = block_values.shape
        values = block_values.reshape(n, 2, tiles * slots // 2, width)
        counts = block_count[0].transpose(1, 2, 0).reshape(tiles * slots, n)
        picks = block_sample[0].transpose(1, 2, 0).reshape(tiles * slots, n)
        weights = sample_weight.reshape(n, -1)
        vmem = pl.BlockSpec(memory_space=pltpu.VMEM)
        anywhere = pl.BlockSpec(memory_space=pl.ANY)
        half = samples // n // 2
        update, scales = pl.pallas_call(
            functools.partial(kernel, n, samples * n, tiles * width * n),
            out_shape=(
                jax.ShapeDtypeStruct((rank, tiles * width), F32),
                jax.ShapeDtypeStruct((1, 128), F32),
            ),
            in_specs=[anywhere] * 8,
            out_specs=(anywhere, vmem),
            scratch_shapes=[
                pltpu.SMEM((samples,), jnp.int32),
                pltpu.SMEM((samples,), jnp.int32),
                pltpu.SMEM(picks.shape, jnp.int32),
                pltpu.VMEM(counts.shape, jnp.int32),
                pltpu.VMEM(factor_b.shape, BF16),
                pltpu.VMEM(factor_c.shape, BF16),
                pltpu.VMEM(weights.shape, F32),
                pltpu.VMEM(values.shape, BF16),
                pltpu.VMEM((factor_c.shape[1], 128), F32),
                pltpu.VMEM((factor_b.shape[1], 128), F32),
                pltpu.VMEM((half, 128), F32),
                pltpu.VMEM((n, half, 128), BF16),
                pltpu.VMEM((n, half, 128), BF16),
                pltpu.VMEM((n, half, 128), F32),
                pltpu.VMEM((n, half, 128), F32),
                pltpu.VMEM((samples, 128), F32),
                pltpu.VMEM((n, 3, 8, 128), BF16),
                pltpu.VMEM((n, 3, 8, 128), BF16),
                pltpu.VMEM((8, 4, 128), F32),
                pltpu.VMEM((8, 4, 128), F32),
                pltpu.VMEM((4, 128), F32),
                pltpu.VMEM((8, 4, 128), F32),
                pltpu.VMEM((4, 128), F32),
                pltpu.VMEM((8, 4, 128), F32),
                pltpu.VMEM((1, 128), F32),
                pltpu.VMEM((n, 1, 128), F32),
                pltpu.VMEM((rank, tiles * width), F32),
                pltpu.SemaphoreType.DMA((9,)),
                pltpu.SemaphoreType.DMA((n,)),
            ]
            + [pltpu.SemaphoreType.DMA(())] * 5
            + [pltpu.SemaphoreType.DMA((3, 8))] * 2,
            compiler_params=pltpu.CompilerParams(collective_id=0, has_side_effects=True),
            name="step",
        )(
            sample_k.reshape(-1),
            sample_j,
            picks,
            counts,
            factor_b,
            factor_c,
            weights,
            values,
        )
        scales = scales[0, :rank]
        return (update / scales[:, None]).astype(BF16), scales

    return jax.shard_map(
        shards,
        mesh=mesh,
        in_specs=(
            P(None, GROUPS_ROW),
            P(None, GROUPS_ROW),
            P(GROUPS_ROW),
            P(None, GROUPS_ROW, None),
            P(GROUPS_ROW),
            P(GROUPS_ROW, None, None, None, None),
            P(GROUPS_ROW, None, None, None),
            P(GROUPS_ROW, None, None, None),
        ),
        out_specs=(P(None, GROUPS_ROW), P("groups")),
        check_vma=False,
    )
```
